32 devices in a mesh: section: 8 (over z, y), state: 4 (over x, core).
Axes of the slice: x: 2, y: 2, z: 4, core: 2. Of those that a mesh axis runs over, the one named last changes fastest.
Arguments:
- initial_state: float32 [32, 1024], P('state'), may hold values from -6 to 6
- state_ref: float32 [192, 32, 1024], P('section', 'state'), may hold values from -6 to 6
- state_weight: float32 [192, 32, 1024], P('section', 'state'), may hold values from 0.2 to 5
- input_matrix: bfloat16 [32, 1024, 512], P('state'), may hold values from -0.25 to 0.25
- kkt_inverse: float32 [512, 512], replicated, may hold values from -1 to 1, as said below
- input_bound: float32 [512], replicated, may hold values from 0.02 to 0.3
Outputs:
- states: float32 [192, 32, 1024], P('section', 'state')
- boxed: float32 [192, 512], P('section')
- dual_vars: float32 [192, 32, 1024], P('section', 'state')
- history: float32 [10, 2], replicated
The draws below stay inside these ranges and needn't reach their ends.
Inputs may be any that keep to these rules, and one draw needn't show every extreme that they name: `kkt_inverse`: a symmetric matrix.
All inputs are finite; a program needn't handle non-finite values.
Results may differ from the reference program's by a relative error of at most 0.003.
Values may be sent and summed in bfloat16 or wider, within the bound.
No kernel may reach another device: no remote copies, remote signals or barrier semaphores. Data moves between devices by JAX's collectives and lax.ppermute only.
A program may use at most 128 MiB of HBM per device.

```python
import math
import jax
import jax.numpy as jnp
from jax import lax

GX = 32
GY = 32
GZ = 32
NU = 512
ITERS = 10
PLANE = 1024
HORIZON = 192


def draw_kkt_inverse(key, part):
    noise_key = jax.random.fold_in(key, 7)
    noise = jax.random.normal(noise_key, (NU, NU), jnp.float32)
    symmetric = (noise + noise.T) * (0.25 / (2.0 * NU) ** 0.5)
    factor = 1.0 / (1.0 + 2.0 * GX * GY * GZ / NU)
    return factor * (jnp.eye(NU, dtype=jnp.float32) + symmetric)


def block_scale(own_key, extent, cuts, low, largest):
    gain = 1.0
    for dim, parts in cuts:
        steps = jax.random.uniform(jax.random.fold_in(jax.random.fold_in(own_key, 6), dim), (parts,), jnp.float32, low / len(cuts), largest / len(cuts))
        gain = gain * jnp.repeat(jnp.exp(steps), extent[dim] // parts).reshape((-1,) + (1,) * (len(extent) - 1 - dim))
    return gain


def bell_draw(own_key, extent, width, bound, split=(), kind=jnp.bfloat16):
    array = width * jax.random.normal(own_key, extent, jnp.float32)
    if split:
        array = array * block_scale(own_key, extent, split, -0.22, 0.18)
    return jnp.clip(array, -bound, bound).astype(kind)


def setup_inputs(seed: int = 0) -> dict:
    seeds = jax.random.split(jax.random.key(seed), 7)
    return {
        "initial_state": bell_draw(seeds[0], (GX, PLANE), 1.0, 6.0, ((0, 4),), jnp.float32),
        "state_ref": bell_draw(seeds[1], (HORIZON, GX, PLANE), 1.0, 6.0, ((0, 8), (1, 4)), jnp.float32),
        "state_weight": jnp.clip(jnp.exp(math.log(5.0) - 3.218876 * jax.random.uniform(seeds[2], (HORIZON, GX, PLANE), jnp.float32) ** block_scale(seeds[2], (HORIZON, GX, PLANE), ((0, 8), (1, 4)), -0.2, 0.2)), 0.2, 5.0),
        "input_matrix": bell_draw(seeds[3], (GX, PLANE, NU), NU ** -0.5, 0.25, ((0, 4),)),
        "kkt_inverse": draw_kkt_inverse(jax.random.fold_in(seeds[6], 71), 0),
        "input_bound": jnp.clip(jnp.exp(jax.random.uniform(seeds[5], (NU,), jnp.float32, math.log(0.02), math.log(0.3))), 0.02, 0.3),
    }


diffusion = 0.15
epsilon = 1e-06

def stencil(padded):
    centre = padded[:, 1:-1]
    across = padded[:, 2:] + padded[:, :-2]
    depth = centre.shape[-1]
    flat_pad = jnp.pad(centre, ((0, 0), (0, 0), (GZ, GZ)))
    along_y = flat_pad[:, :, 2 * GZ:] + flat_pad[:, :, :-2 * GZ]
    lower_z = jnp.pad(centre, ((0, 0), (0, 0), (1, 0)))[:, :, :-1]
    upper_z = jnp.pad(centre, ((0, 0), (0, 0), (0, 1)))[:, :, 1:]
    z_index = jnp.arange(depth) % GZ
    along_z = jnp.where(z_index > 0, lower_z, 0.0) + jnp.where(z_index < GZ - 1, upper_z, 0.0)
    return centre + diffusion * (across + along_y + along_z - 6.0 * centre)

def reference(initial_state, state_ref, state_weight, input_matrix, kkt_inverse, input_bound):
    horizon = state_ref.shape[0]
    cell_total = input_matrix.shape[0] * input_matrix.shape[1]
    input_width = input_matrix.shape[2]
    matrix = input_matrix.reshape(cell_total, input_width)
    penalty = float(cell_total) / input_width
    states = jnp.zeros_like(state_ref)
    dual_vars = jnp.zeros_like(state_ref)
    boxed = jnp.zeros((horizon, input_width), jnp.float32)
    scaled = jnp.zeros((horizon, input_width), jnp.float32)
    history = []
    for iteration in range(ITERS):
        before = jnp.concatenate([initial_state[None], states[:-1]], 0)
        moved_prior = stencil(jnp.pad(before, ((0, 0), (1, 1), (0, 0))))
        target = states - moved_prior + dual_vars
        target_low = target.astype(jnp.bfloat16).reshape(horizon, cell_total)
        pulled = jnp.dot(target_low, matrix, preferred_element_type=jnp.float32)
        rhs_rows = pulled + penalty * (boxed - scaled)
        inputs = jnp.dot(rhs_rows, kkt_inverse, precision=lax.Precision.HIGHEST)
        inputs_low = inputs.astype(jnp.bfloat16)
        driven = jnp.dot(inputs_low, matrix.T, preferred_element_type=jnp.float32).reshape(states.shape)
        defect = target - driven
        ahead_defect = jnp.concatenate([defect[1:], jnp.zeros_like(defect[:1])], 0)
        back_term = stencil(jnp.pad(ahead_defect, ((0, 0), (1, 1), (0, 0))))
        updated = (state_weight * state_ref + (states - defect) + back_term + states) / (state_weight + 2.0)
        primal = updated - moved_prior - driven
        dual_vars = dual_vars + primal
        boxed_new = jnp.clip(inputs + scaled, -input_bound, input_bound)
        box_gap = inputs - boxed_new
        scaled = scaled + box_gap
        boxed = boxed_new
        states = updated
        history.append(jnp.stack([jnp.sqrt(jnp.mean(primal * primal) + epsilon), jnp.sqrt(jnp.mean(box_gap * box_gap) + epsilon)]))
    return (states, boxed, dual_vars, jnp.stack(history))
```

```python
import functools

import jax
import jax.numpy as jnp
from jax import lax
from jax.experimental import pallas as pl
from jax.experimental.pallas import tpu as pltpu
from jax.sharding import PartitionSpec as P

GX = 32
GY = 32
GZ = 32
ITERS = 10
LANES = 128

diffusion = 0.15
epsilon = 1e-06

VMEM_LIMIT = 48 * 1024 * 1024


def xor_pairs(count, mask):
    return [(i, i ^ mask) for i in range(count)]


def odd_masks(count):
    return sorted({i ^ (i + 1) for i in range(1, count - 1, 2)})


def swapped(value, axis, mask):
    return lax.ppermute(value, axis, xor_pairs(lax.axis_size(axis), mask))


def across_odd(values, axis):
    count = lax.axis_size(axis)
    masks = odd_masks(count)
    seat = lax.axis_index(axis)
    result = jnp.zeros_like(values)
    for mask in masks:
        got = swapped(values, axis, mask)
        lower = seat ^ mask
        near = (seat % 2 == 1) & (lower == seat + 1) | (seat % 2 == 0) & (lower + 1 == seat)
        result = jnp.where(near, got, result)
    return result


def bulk_across_odd(value, axis):
    count = lax.axis_size(axis)
    pairs = []
    for i in range(1, count - 1, 2):
        pairs += [(i, i + 1), (i + 1, i)]
    if not pairs:
        return jnp.zeros_like(value)
    return lax.ppermute(value, axis, pairs)


def lane_masks(rows):
    lane = lax.broadcasted_iota(jnp.int32, (rows, LANES), 1)
    return lane < GZ, lane >= LANES - GZ, lane % GZ == 0, lane % GZ == GZ - 1


def stencil_columns(read, columns, masks):
    first_y, last_y, first_z, last_z = masks
    centre = [read(0, j) for j in range(columns)]
    up = [pltpu.roll(c, GZ, 1) for c in centre]
    down = [pltpu.roll(c, LANES - GZ, 1) for c in centre]
    out = []
    for j in range(columns):
        above = up[j - 1] if j > 0 else 0.0
        below = down[j + 1] if j < columns - 1 else 0.0
        total = jnp.where(first_y, above, up[j]) + jnp.where(last_y, below, down[j])
        total += jnp.where(first_z, 0.0, pltpu.roll(centre[j], 1, 1))
        total += jnp.where(last_z, 0.0, pltpu.roll(centre[j], LANES - 1, 1))
        total += read(-1, j) + read(1, j)
        out.append((1.0 - 6.0 * diffusion) * centre[j] + diffusion * total)
    return out


def column(j):
    return slice(j * LANES, (j + 1) * LANES)


def inputs_step(parts, boxed_ref, scaled_ref, bound_ref, kkt_ref, penalty, own):
    sums = [p[...].astype(jnp.float32) for p in parts]
    while len(sums) > 1:
        sums = [sums[i] + sums[i + 1] for i in range(0, len(sums), 2)]
    boxed = boxed_ref[...]
    scaled = scaled_ref[...]
    rhs = sums[0] + penalty * (boxed - scaled)
    inputs = jnp.dot(
        rhs, kkt_ref[...], precision=lax.Precision.HIGHEST, preferred_element_type=jnp.float32
    )
    bound = bound_ref[...]
    boxed_new = jnp.clip(inputs + scaled, -bound, bound)
    gap = inputs - boxed_new
    square = gap * gap
    total = square[0:8]
    for i in range(8, own, 8):
        total = total + square[i : i + 8]
    return inputs, boxed_new, scaled + gap, total


def drive(inputs_low, block):
    return lax.dot_general(
        inputs_low, block, (((1,), (1,)), ((), ())), preferred_element_type=jnp.float32
    )


def defect_planes(
    flags, inputs_low, matrix_ref, near_ref, far_ref, target_ref, near_rim, far_rim, defect_ref
):
    planes = target_ref.shape[0]

    def own_plane(p, _):
        defect_ref[p + 2] = target_ref[p] - drive(inputs_low, matrix_ref[p])
        return 0

    lax.fori_loop(0, planes, own_plane, 0)
    even = flags[0]
    keep = flags[1].astype(jnp.float32)
    near_base = even * (planes + 2)
    far_base = (1 - even) * (planes + 2)
    for i in range(2):
        defect_ref[near_base + i] = near_rim[i].astype(jnp.float32) - drive(inputs_low, near_ref[i])
        defect_ref[far_base + i] = keep * (
            far_rim[i].astype(jnp.float32) - drive(inputs_low, far_ref[i])
        )


def step_kernel(groups, own, halo, penalty, with_extra, *refs):
    refs = list(refs)
    flags = refs.pop(0)
    parts = [refs.pop(0) for _ in range(groups)]
    boxed_ref, scaled_ref, bound_ref, kkt_ref = [refs.pop(0) for _ in range(4)]
    matrix_ref, near_ref, far_ref = [refs.pop(0) for _ in range(3)]
    target_ref, near_rim, far_rim = [refs.pop(0) for _ in range(3)]
    states_ref, duals_ref, inverse_ref, goal_ref = [refs.pop(0) for _ in range(4)]
    extra_ref = refs.pop(0) if with_extra else None
    boxed_out, scaled_out, states_out, duals_out, target_out = [refs.pop(0) for _ in range(5)]
    part_out, near_out, far_out, primal_out, gap_out = [refs.pop(0) for _ in range(5)]
    defect_ref, low_ref = refs

    planes, rows, plane_size = target_ref.shape
    columns = plane_size // LANES
    inputs, boxed_new, scaled_new, gap_total = inputs_step(
        parts, boxed_ref, scaled_ref, bound_ref, kkt_ref, penalty, own
    )
    boxed_out[...] = boxed_new
    scaled_out[...] = scaled_new
    gap_out[...] = gap_total
    inputs_low = inputs.astype(jnp.bfloat16)
    defect_planes(
        flags, inputs_low, matrix_ref, near_ref, far_ref, target_ref, near_rim, far_rim, defect_ref
    )
    masks = lane_masks(rows)

    def new_states(q, keep_duals, total):
        def read(offset, j):
            return defect_ref[q + 1 + offset, :, column(j)]

        spread = stencil_columns(read, columns, masks)
        for j in range(columns):
            ahead = pltpu.roll(spread[j], rows - 1, 0)
            defect = defect_ref[q + 1, :, column(j)]
            old = states_ref[q, :, column(j)]
            new = goal_ref[q, :, column(j)] + inverse_ref[q, :, column(j)] * (
                (old - defect) + ahead + old
            )
            states_out[q, :, column(j)] = new
            if keep_duals:
                dual = (new - old) + defect
                primal = dual - duals_ref[q - 1, :, column(j)]
                duals_out[q - 1, :, column(j)] = dual
                square = primal * primal
                for i in range(0, own, 8):
                    total = total + square[i : i + 8]
        return total

    zero = jnp.zeros((8, LANES), jnp.float32)
    new_states(0, False, zero)
    new_states(planes + 1, False, zero)
    primal_out[...] = lax.fori_loop(
        1, planes + 1, lambda q, total: new_states(q, True, total), zero
    )

    row = lax.broadcasted_iota(jnp.int32, (rows, LANES), 0)
    live = (row < own) | (row < own + halo) & (flags[3] == 0) | (row >= own + halo) & (flags[2] == 0)

    def new_target(p, total):
        def read(offset, j):
            return states_out[p + 1 + offset, :, column(j)]

        spread = stencil_columns(read, columns, masks)
        for j in range(columns):
            moved = pltpu.roll(spread[j], 1, 0)
            if with_extra:
                moved = jnp.where(row == own + halo, extra_ref[p, 0:1, column(j)], moved)
            new = (states_out[p + 1, :, column(j)] - moved) + duals_out[p, :, column(j)]
            new = jnp.where(live, new, 0.0)
            target_out[p, :, column(j)] = new
            low_ref[p, :, column(j)] = new.astype(jnp.bfloat16)
        return total + jnp.dot(low_ref[p], matrix_ref[p], preferred_element_type=jnp.float32)

    width = matrix_ref.shape[2]
    part = lax.fori_loop(0, planes, new_target, jnp.zeros((rows, width), jnp.float32))
    part_out[...] = part.astype(jnp.bfloat16)
    near_base = flags[0] * (planes - 2)
    far_base = (1 - flags[0]) * (planes - 2)
    for i in range(2):
        near_out[i] = low_ref[near_base + i]
        far_out[i] = low_ref[far_base + i]


def last_inputs_kernel(groups, own, penalty, *refs):
    refs = list(refs)
    flags = refs.pop(0)
    parts = [refs.pop(0) for _ in range(groups)]
    boxed_ref, scaled_ref, bound_ref, kkt_ref = [refs.pop(0) for _ in range(4)]
    matrix_ref, near_ref, far_ref = [refs.pop(0) for _ in range(3)]
    target_ref, near_rim, far_rim = [refs.pop(0) for _ in range(3)]
    boxed_out, gap_out, defect_out, first_out = refs
    inputs, boxed_new, _, gap_total = inputs_step(
        parts, boxed_ref, scaled_ref, bound_ref, kkt_ref, penalty, own
    )
    boxed_out[...] = boxed_new
    gap_out[...] = gap_total
    defect_planes(
        flags,
        inputs.astype(jnp.bfloat16),
        matrix_ref,
        near_ref,
        far_ref,
        target_ref,
        near_rim,
        far_rim,
        defect_out,
    )
    first_out[...] = defect_out[:, 0:8, :]


def last_states_kernel(
    own, defect_ref, following_ref, states_ref, duals_ref, inverse_ref, goal_ref, *outs
):
    states_out, duals_out, primal_out = outs
    planes = states_out.shape[0]
    columns = states_out.shape[2] // LANES
    masks = lane_masks(own)
    last = lax.broadcasted_iota(jnp.int32, (own, LANES), 0) == own - 1

    def body(p, total):
        def read(offset, j):
            own_rows = defect_ref[p + 2 + offset, 0:own, column(j)]
            after = following_ref[p + 2 + offset, 0:1, column(j)]
            return jnp.where(last, after, pltpu.roll(own_rows, own - 1, 0))

        spread = stencil_columns(read, columns, masks)
        for j in range(columns):
            defect = defect_ref[p + 2, 0:own, column(j)]
            old = states_ref[p + 1, 0:own, column(j)]
            new = goal_ref[p + 1, 0:own, column(j)] + inverse_ref[p + 1, 0:own, column(j)] * (
                (old - defect) + spread[j] + old
            )
            dual = (new - old) + defect
            primal = dual - duals_ref[p, 0:own, column(j)]
            states_out[p, :, column(j)] = new
            duals_out[p, :, column(j)] = dual
            square = primal * primal
            for i in range(0, own, 8):
                total = total + square[i : i + 8]
        return total

    primal_out[...] = lax.fori_loop(0, planes, body, jnp.zeros((8, LANES), jnp.float32))


def in_vmem(count):
    return [pl.BlockSpec(memory_space=pltpu.VMEM)] * count


def call(kernel, flags, operands, outs, scratch=(), flops=0):
    specs = in_vmem(len(operands))
    if flags is not None:
        specs = [pl.BlockSpec(memory_space=pltpu.SMEM)] + specs
        operands = (flags, *operands)
    return pl.pallas_call(
        kernel,
        out_shape=outs,
        in_specs=specs,
        out_specs=tuple(in_vmem(len(outs))),
        scratch_shapes=list(scratch),
        compiler_params=pltpu.CompilerParams(vmem_limit_bytes=VMEM_LIMIT),
        cost_estimate=pl.CostEstimate(flops=flops, bytes_accessed=30_000_000, transcendentals=0),
    )(*operands)


def all_sum(value, axis):
    mask = 1
    while mask < lax.axis_size(axis):
        value = value + swapped(value, axis, mask)
        mask *= 2
    return value


def local(initial_state, state_ref, state_weight, input_matrix, kkt_inverse, input_bound):
    own, planes, plane_size = state_ref.shape
    width = input_matrix.shape[2]
    halo = ITERS - 2
    rows = own + 2 * halo
    assert own > halo and own % 8 == 0 and halo % 8 == 0 and plane_size == GY * GZ
    penalty = float(GX * GY * GZ) / width
    groups = lax.axis_size("state")
    sections = lax.axis_size("section")
    seat = lax.axis_index("state")
    section = lax.axis_index("section")
    even = seat % 2 == 0
    even_section = section % 2 == 0
    is_first = section == 0
    is_last = section == sections - 1
    far_lives = jnp.logical_not((seat == 0) | (seat == groups - 1) & (groups % 2 == 0))
    flags = jnp.stack(
        [even.astype(jnp.int32), far_lives.astype(jnp.int32), is_first.astype(jnp.int32), is_last.astype(jnp.int32)]
    )

    top = input_matrix[planes - 2 :]
    bottom = input_matrix[:2]
    near_matrix = swapped(jnp.where(even, top, bottom), "state", 1)
    far_matrix = across_odd(jnp.where(even, bottom, top), "state")

    inverse = 1.0 / (state_weight + 2.0)
    goal = state_weight * state_ref * inverse
    both = jnp.stack([goal, inverse]).transpose(0, 2, 1, 3)
    to_next = both[:, :, own - halo - 1 :]
    to_previous = both[:, :, : halo + 1]
    paired = swapped(jnp.where(even_section, to_next, to_previous).astype(jnp.bfloat16), "section", 1)
    other = bulk_across_odd(
        jnp.where(even_section, to_previous, to_next).astype(jnp.bfloat16), "section"
    )
    paired = paired.astype(jnp.float32)
    other = other.astype(jnp.float32)
    from_next = jnp.where(even_section, paired, other)
    from_previous = jnp.where(even_section, other, paired)
    pinned = jnp.concatenate(
        [jnp.zeros((planes, halo, plane_size), jnp.float32), initial_state[:, None]], 1
    )
    pinned = jnp.stack([pinned, jnp.zeros_like(pinned)])
    from_previous = jnp.where(is_first, pinned, from_previous)
    wide = jnp.concatenate(
        [both, from_next[:, :, :halo], from_previous[:, :, 1:], from_previous[:, :, :1]], 2
    )
    near_plane = swapped(jnp.where(even, wide[:, planes - 1], wide[:, 0]), "state", 1)
    far_plane = across_odd(jnp.where(even, wide[:, 0], wide[:, planes - 1]), "state")
    far_plane = jnp.where(far_lives, far_plane, 0.0)
    low_plane = jnp.where(even, far_plane, near_plane)
    high_plane = jnp.where(even, near_plane, far_plane)
    wide = jnp.concatenate([low_plane[:, None], wide, high_plane[:, None]], 1)
    goal = wide[0, :, :rows]
    inverse = wide[1, :, :rows]
    extra = wide[0, :, rows]

    near_state = swapped(jnp.where(even, initial_state[planes - 1], initial_state[0]), "state", 1)
    far_state = across_odd(jnp.where(even, initial_state[0], initial_state[planes - 1]), "state")
    far_state = jnp.where(far_lives, far_state, 0.0)
    low_state = jnp.where(even, far_state, near_state)
    high_state = jnp.where(even, near_state, far_state)

    def stencil(padded):
        centre = padded[1:-1]
        grid = centre.reshape(-1, GY, GZ)
        total = padded[2:] + padded[:-2]
        in_y = jnp.pad(grid, ((0, 0), (1, 1), (0, 0)))
        in_z = jnp.pad(grid, ((0, 0), (0, 0), (1, 1)))
        total += (in_y[:, 2:] + in_y[:, :-2] + in_z[:, :, 2:] + in_z[:, :, :-2]).reshape(centre.shape)
        return (1.0 - 6.0 * diffusion) * centre + diffusion * total

    moved = stencil(jnp.concatenate([low_state[None], initial_state, high_state[None]]))
    extra_moved = jnp.broadcast_to(stencil(extra)[:, None], (planes, 8, plane_size))
    first = jnp.where(is_first, -moved, 0.0)
    target = jnp.concatenate(
        [first[:, None], jnp.zeros((planes, rows - 1, plane_size), jnp.float32)], 1
    )
    first_low = first.astype(jnp.bfloat16)
    first_part = jnp.dot(
        jnp.broadcast_to(first_low.reshape(1, -1), (8, planes * plane_size)),
        input_matrix.reshape(planes * plane_size, width),
        preferred_element_type=jnp.float32,
    )
    part = jnp.concatenate(
        [first_part[:1], jnp.zeros((rows - 1, width), jnp.float32)], 0
    ).astype(jnp.bfloat16)
    rims = target.astype(jnp.bfloat16)
    near_rim = jnp.where(even, rims[planes - 2 :], rims[:2])
    far_rim = jnp.where(even, rims[:2], rims[planes - 2 :])

    states = jnp.zeros((planes + 2, rows, plane_size), jnp.float32)
    duals = jnp.zeros((planes, rows, plane_size), jnp.float32)
    boxed = jnp.zeros((rows, width), jnp.float32)
    scaled = jnp.zeros((rows, width), jnp.float32)
    bound = input_bound.reshape(1, width)

    f32 = jnp.float32
    shape = jax.ShapeDtypeStruct
    vector = shape((8, LANES), f32)
    small = shape((rows, width), f32)
    rim_shape = shape((2, rows, plane_size), jnp.bfloat16)
    flops = 4 * rows * width * planes * plane_size
    primals = []
    gaps = []
    for iteration in range(ITERS):
        parts = [part] + [swapped(part, "state", mask) for mask in range(1, groups)]
        near_in = swapped(near_rim, "state", 1)
        far_in = across_odd(far_rim, "state")
        head = (*parts, boxed, scaled, bound, kkt_inverse, input_matrix, near_matrix, far_matrix)
        head = (*head, target, near_in, far_in)
        if iteration < ITERS - 1:
            with_extra = iteration == 0
            tail = (states, duals, inverse, goal) + ((extra_moved,) if with_extra else ())
            outs = (
                small,
                small,
                shape(states.shape, f32),
                shape(duals.shape, f32),
                shape(target.shape, f32),
                shape((rows, width), jnp.bfloat16),
                rim_shape,
                rim_shape,
                vector,
                shape((8, width), f32),
            )
            boxed, scaled, states, duals, target, part, near_rim, far_rim, primal, gap = call(
                functools.partial(step_kernel, groups, own, halo, penalty, with_extra),
                flags,
                head + tail,
                outs,
                [
                    pltpu.VMEM((planes + 4, rows, plane_size), f32),
                    pltpu.VMEM((planes, rows, plane_size), jnp.bfloat16),
                ],
                flops,
            )
        else:
            defect_shape = (planes + 4, rows, plane_size)
            boxed, gap, defect, edge = call(
                functools.partial(last_inputs_kernel, groups, own, penalty),
                flags,
                head,
                (
                    small,
                    shape((8, width), f32),
                    shape(defect_shape, f32),
                    shape((planes + 4, 8, plane_size), f32),
                ),
                (),
                flops // 2,
            )
            edge = edge[:, 0]
            following = jnp.where(
                even_section, swapped(edge, "section", 1), across_odd(edge, "section")
            )
            following = jnp.where(is_last, 0.0, following)
            following = jnp.broadcast_to(following[:, None], (planes + 4, 8, plane_size))
            own_shape = shape((planes, own, plane_size), f32)
            states, duals, primal = call(
                functools.partial(last_states_kernel, own),
                None,
                (defect, following, states, duals, inverse, goal),
                (own_shape, own_shape, vector),
                (),
                1_000_000,
            )
        primals.append(primal)
        gaps.append(gap)

    primal_square = jnp.sum(jnp.stack(primals), (1, 2))
    gap_square = jnp.sum(jnp.stack(gaps), (1, 2)) / groups
    totals = jnp.stack([primal_square, gap_square], 1)
    totals = jnp.pad(totals.reshape(1, -1), ((0, 7), (0, LANES - 2 * ITERS)))
    totals = all_sum(all_sum(totals, "state"), "section")
    totals = totals[0, : 2 * ITERS].reshape(ITERS, 2)
    total_sections = own * sections
    counts = jnp.array([total_sections * GX * GY * GZ, total_sections * width], f32)
    record = jnp.sqrt(totals / counts + epsilon)
    return (
        states.transpose(1, 0, 2),
        boxed[:own],
        duals.transpose(1, 0, 2),
        record,
    )


def solution(mesh):
    return jax.shard_map(
        local,
        mesh=mesh,
        in_specs=(
            P("state", None),
            P("section", "state", None),
            P("section", "state", None),
            P("state", None, None),
            P(),
            P(),
        ),
        out_specs=(
            P("section", "state", None),
            P("section", None),
            P("section", "state", None),
            P(),
        ),
        check_vma=False,
    )
```

```python
import functools

import jax
import jax.numpy as jnp
from jax import lax
from jax.experimental import pallas as pl
from jax.experimental.pallas import tpu as pltpu
from jax.sharding import PartitionSpec as P

GX = 32
GY = 32
GZ = 32
ITERS = 10
LANES = 128

diffusion = 0.15
epsilon = 1e-06

VMEM_LIMIT = 14 * 1024 * 1024


def xor_pairs(count, mask):
    return [(i, i ^ mask) for i in range(count)]


def odd_masks(count):
    return sorted({i ^ (i + 1) for i in range(1, count - 1, 2)})


def swapped(value, axis, mask):
    return lax.ppermute(value, axis, xor_pairs(lax.axis_size(axis), mask))


def across_odd(values, axis):
    count = lax.axis_size(axis)
    masks = odd_masks(count)
    seat = lax.axis_index(axis)
    result = jnp.zeros_like(values)
    for mask in masks:
        got = swapped(values, axis, mask)
        lower = seat ^ mask
        near = (seat % 2 == 1) & (lower == seat + 1) | (seat % 2 == 0) & (lower + 1 == seat)
        result = jnp.where(near, got, result)
    return result


def bulk_across_odd(value, axis):
    count = lax.axis_size(axis)
    pairs = []
    for i in range(1, count - 1, 2):
        pairs += [(i, i + 1), (i + 1, i)]
    if not pairs:
        return jnp.zeros_like(value)
    return lax.ppermute(value, axis, pairs)


def lane_masks(rows):
    lane = lax.broadcasted_iota(jnp.int32, (rows, LANES), 1)
    return lane < GZ, lane >= LANES - GZ, lane % GZ == 0, lane % GZ == GZ - 1


def stencil_columns(read, columns, masks):
    first_y, last_y, first_z, last_z = masks
    centre = read(0, 0)
    above = 0.0
    up = pltpu.roll(centre, GZ, 1)
    down = pltpu.roll(centre, LANES - GZ, 1)
    for j in range(columns):
        if j < columns - 1:
            centre_next = read(0, j + 1)
            up_next = pltpu.roll(centre_next, GZ, 1)
            down_next = pltpu.roll(centre_next, LANES - GZ, 1)
            below = down_next
        else:
            below = 0.0
        total = jnp.where(first_y, above, up) + jnp.where(last_y, below, down)
        total += jnp.where(first_z, 0.0, pltpu.roll(centre, 1, 1))
        total += jnp.where(last_z, 0.0, pltpu.roll(centre, LANES - 1, 1))
        total += read(-1, j) + read(1, j)
        yield j, centre, (1.0 - 6.0 * diffusion) * centre + diffusion * total
        if j < columns - 1:
            above, centre, up, down = up, centre_next, up_next, down_next


def column(j):
    return slice(j * LANES, (j + 1) * LANES)


def inputs_step(parts, boxed_ref, scaled_ref, bound_ref, kkt_ref, penalty, own):
    sums = [p[...].astype(jnp.float32) for p in parts]
    while len(sums) > 1:
        sums = [sums[i] + sums[i + 1] for i in range(0, len(sums), 2)]
    boxed = boxed_ref[...]
    scaled = scaled_ref[...]
    rhs = sums[0] + penalty * (boxed - scaled)
    inputs = jnp.dot(
        rhs, kkt_ref[...], precision=lax.Precision.HIGHEST, preferred_element_type=jnp.float32
    )
    bound = bound_ref[...]
    boxed_new = jnp.clip(inputs + scaled, -bound, bound)
    gap = inputs - boxed_new
    square = gap * gap
    total = square[0:8]
    for i in range(8, own, 8):
        total = total + square[i : i + 8]
    return inputs, boxed_new, scaled + gap, total


def drive(inputs_low, block):
    return jnp.dot(inputs_low, block, preferred_element_type=jnp.float32)


def rim_defects(flags, inputs_low, near_ref, far_ref, planes, near_rim, far_rim, defect_ref):
    even = flags[0]
    keep = flags[1].astype(jnp.float32)
    near_base = even * (planes + 2)
    far_base = (1 - even) * (planes + 2)
    for i in range(2):
        defect_ref[near_base + i] = near_rim[i].astype(jnp.float32) - drive(inputs_low, near_ref[i])
        defect_ref[far_base + i] = keep * (
            far_rim[i].astype(jnp.float32) - drive(inputs_low, far_ref[i])
        )


def step_kernel(groups, own, halo, penalty, with_extra, *refs):
    refs = list(refs)
    flags = refs.pop(0)
    parts = [refs.pop(0) for _ in range(groups)]
    boxed_ref, scaled_ref, bound_ref, kkt_ref = [refs.pop(0) for _ in range(4)]
    matrix_ref, turned_ref, near_ref, far_ref = [refs.pop(0) for _ in range(4)]
    target_ref, near_rim, far_rim = [refs.pop(0) for _ in range(3)]
    states_ref, duals_ref, inverse_ref, goal_ref = [refs.pop(0) for _ in range(4)]
    extra_ref = refs.pop(0) if with_extra else None
    boxed_out, scaled_out, states_out, duals_out, target_out = [refs.pop(0) for _ in range(5)]
    part_out, near_out, far_out, primal_out, gap_out = [refs.pop(0) for _ in range(5)]
    defect_ref, low_ref = refs

    planes, rows, plane_size = target_ref.shape
    columns = plane_size // LANES
    inputs, boxed_new, scaled_new, gap_total = inputs_step(
        parts, boxed_ref, scaled_ref, bound_ref, kkt_ref, penalty, own
    )
    boxed_out[...] = boxed_new
    scaled_out[...] = scaled_new
    gap_out[...] = gap_total
    inputs_low = inputs.astype(jnp.bfloat16)
    rim_defects(flags, inputs_low, near_ref, far_ref, planes, near_rim, far_rim, defect_ref)
    masks = lane_masks(rows)

    def own_defect(p):
        defect_ref[p + 2] = target_ref[p] - drive(inputs_low, turned_ref[p])

    def new_states(q, keep_duals, total):
        def read(offset, j):
            return defect_ref[q + 1 + offset, :, column(j)]

        for j, defect, spread in stencil_columns(read, columns, masks):
            ahead = pltpu.roll(spread, rows - 1, 0)
            old = states_ref[q, :, column(j)]
            new = goal_ref[q, :, column(j)] + inverse_ref[q, :, column(j)] * (
                (old - defect) + ahead + old
            )
            states_out[q, :, column(j)] = new
            if keep_duals:
                dual = (new - old) + defect
                primal = dual - duals_ref[q - 1, :, column(j)]
                duals_out[q - 1, :, column(j)] = dual
                square = primal * primal
                for i in range(0, own, 8):
                    total = total + square[i : i + 8]
        return total

    def states_and_defect(q, total):
        total = new_states(q, True, total)
        own_defect(q + 1)
        return total

    total = jnp.zeros((8, LANES), jnp.float32)
    own_defect(0)
    own_defect(1)
    new_states(0, False, total)
    total = lax.fori_loop(1, planes - 1, states_and_defect, total)
    total = lax.fori_loop(
        planes - 1, planes + 1, lambda q, total: new_states(q, True, total), total
    )
    new_states(planes + 1, False, total)
    primal_out[...] = total

    row = lax.broadcasted_iota(jnp.int32, (rows, LANES), 0)
    live = (row < own) | (row < own + halo) & (flags[3] == 0) | (row >= own + halo) & (flags[2] == 0)

    def new_target(p):
        def read(offset, j):
            return states_out[p + 1 + offset, :, column(j)]

        for j, centre, spread in stencil_columns(read, columns, masks):
            moved = pltpu.roll(spread, 1, 0)
            if with_extra:
                moved = jnp.where(row == own + halo, extra_ref[p, 0:1, column(j)], moved)
            new = (centre - moved) + duals_out[p, :, column(j)]
            new = jnp.where(live, new, 0.0)
            target_out[p, :, column(j)] = new
            low_ref[p, :, column(j)] = new.astype(jnp.bfloat16)

    def pull(p):
        return jnp.dot(low_ref[p], matrix_ref[p], preferred_element_type=jnp.float32)

    def pull_and_target(p, part):
        part = part + pull(p - 1)
        new_target(p)
        return part

    width = matrix_ref.shape[2]
    new_target(0)
    part = lax.fori_loop(1, planes, pull_and_target, jnp.zeros((rows, width), jnp.float32))
    part_out[...] = (part + pull(planes - 1)).astype(jnp.bfloat16)
    near_base = flags[0] * (planes - 2)
    far_base = (1 - flags[0]) * (planes - 2)
    for i in range(2):
        near_out[i] = low_ref[near_base + i]
        far_out[i] = low_ref[far_base + i]


def last_inputs_kernel(groups, own, penalty, *refs):
    refs = list(refs)
    flags = refs.pop(0)
    parts = [refs.pop(0) for _ in range(groups)]
    boxed_ref, scaled_ref, bound_ref, kkt_ref = [refs.pop(0) for _ in range(4)]
    turned_ref, near_ref, far_ref = [refs.pop(0) for _ in range(3)]
    target_ref, near_rim, far_rim = [refs.pop(0) for _ in range(3)]
    boxed_out, gap_out, defect_out, first_out = refs
    inputs, boxed_new, _, gap_total = inputs_step(
        parts, boxed_ref, scaled_ref, bound_ref, kkt_ref, penalty, own
    )
    boxed_out[...] = boxed_new
    gap_out[...] = gap_total
    inputs_low = inputs.astype(jnp.bfloat16)
    planes = target_ref.shape[0]
    rim_defects(flags, inputs_low, near_ref, far_ref, planes, near_rim, far_rim, defect_out)

    def own_defect(p, _):
        defect_out[p + 2] = target_ref[p] - drive(inputs_low, turned_ref[p])
        return 0

    lax.fori_loop(0, planes, own_defect, 0)
    first_out[...] = defect_out[:, 0:8, :]


def last_states_kernel(
    own, defect_ref, following_ref, states_ref, duals_ref, inverse_ref, goal_ref, *outs
):
    states_out, duals_out, primal_out = outs
    planes = states_out.shape[0]
    columns = states_out.shape[2] // LANES
    masks = lane_masks(own)
    last = lax.broadcasted_iota(jnp.int32, (own, LANES), 0) == own - 1

    def body(p, total):
        def read(offset, j):
            own_rows = defect_ref[p + 2 + offset, 0:own, column(j)]
            after = following_ref[p + 2 + offset, 0:1, column(j)]
            return jnp.where(last, after, pltpu.roll(own_rows, own - 1, 0))

        for j, _, spread in stencil_columns(read, columns, masks):
            defect = defect_ref[p + 2, 0:own, column(j)]
            old = states_ref[p + 1, 0:own, column(j)]
            new = goal_ref[p + 1, 0:own, column(j)] + inverse_ref[p + 1, 0:own, column(j)] * (
                (old - defect) + spread + old
            )
            dual = (new - old) + defect
            primal = dual - duals_ref[p, 0:own, column(j)]
            states_out[p, :, column(j)] = new
            duals_out[p, :, column(j)] = dual
            square = primal * primal
            for i in range(0, own, 8):
                total = total + square[i : i + 8]
        return total

    primal_out[...] = lax.fori_loop(0, planes, body, jnp.zeros((8, LANES), jnp.float32))


def in_vmem(count):
    return [pl.BlockSpec(memory_space=pltpu.VMEM)] * count


def call(kernel, flags, operands, outs, scratch=(), flops=0):
    specs = in_vmem(len(operands))
    if flags is not None:
        specs = [pl.BlockSpec(memory_space=pltpu.SMEM)] + specs
        operands = (flags, *operands)
    return pl.pallas_call(
        kernel,
        out_shape=outs,
        in_specs=specs,
        out_specs=tuple(in_vmem(len(outs))),
        scratch_shapes=list(scratch),
        compiler_params=pltpu.CompilerParams(vmem_limit_bytes=VMEM_LIMIT),
        cost_estimate=pl.CostEstimate(flops=flops, bytes_accessed=30_000_000, transcendentals=0),
    )(*operands)


def all_sum(value, axis):
    mask = 1
    while mask < lax.axis_size(axis):
        value = value + swapped(value, axis, mask)
        mask *= 2
    return value


def local(initial_state, state_ref, state_weight, input_matrix, kkt_inverse, input_bound):
    own, planes, plane_size = state_ref.shape
    width = input_matrix.shape[2]
    halo = ITERS - 2
    rows = own + 2 * halo
    assert own > halo and own % 8 == 0 and halo % 8 == 0 and plane_size == GY * GZ
    penalty = float(GX * GY * GZ) / width
    groups = lax.axis_size("state")
    sections = lax.axis_size("section")
    seat = lax.axis_index("state")
    section = lax.axis_index("section")
    even = seat % 2 == 0
    even_section = section % 2 == 0
    is_first = section == 0
    is_last = section == sections - 1
    far_lives = jnp.logical_not((seat == 0) | (seat == groups - 1) & (groups % 2 == 0))
    flags = jnp.stack(
        [even.astype(jnp.int32), far_lives.astype(jnp.int32), is_first.astype(jnp.int32), is_last.astype(jnp.int32)]
    )

    def costs(weight, goal):
        inverse = 1.0 / (weight + 2.0)
        return weight * goal * inverse, inverse

    def rim_costs(plane):
        return jnp.concatenate(
            [*costs(state_weight[:, plane], state_ref[:, plane]), initial_state[plane : plane + 1]]
        )

    above = rim_costs(planes - 1)
    below = rim_costs(0)
    near_plane = swapped(jnp.where(even, above, below).astype(jnp.bfloat16), "state", 1)
    far_plane = across_odd(jnp.where(even, below, above).astype(jnp.bfloat16), "state")

    base = jnp.where(even, planes - 2, 0)
    near_matrix = swapped(lax.dynamic_slice_in_dim(input_matrix, base, 2), "state", 1)
    far_matrix = bulk_across_odd(
        lax.dynamic_slice_in_dim(input_matrix, planes - 2 - base, 2), "state"
    )

    def turned(matrix):
        return matrix.transpose(0, 2, 1)

    near_plane = near_plane.astype(jnp.float32)
    far_plane = jnp.where(far_lives, far_plane.astype(jnp.float32), 0.0)
    low_plane = jnp.where(even, far_plane, near_plane)
    high_plane = jnp.where(even, near_plane, far_plane)

    def with_rims(low, block, high):
        return jnp.concatenate([low[None], block, high[None]])

    goal, inverse = costs(state_weight, state_ref)
    goal = with_rims(low_plane[:own], goal.transpose(1, 0, 2), high_plane[:own])
    inverse = with_rims(
        low_plane[own : 2 * own], inverse.transpose(1, 0, 2), high_plane[own : 2 * own]
    )
    initial = with_rims(low_plane[2 * own], initial_state, high_plane[2 * own])

    def message(first, stop):
        return jnp.stack([goal[:, first:stop], inverse[:, first:stop]]).astype(jnp.bfloat16)

    to_next = message(own - halo - 1, own)
    to_previous = message(0, halo + 1)
    paired = swapped(jnp.where(even_section, to_next, to_previous), "section", 1)
    other = bulk_across_odd(jnp.where(even_section, to_previous, to_next), "section")
    from_next = jnp.where(even_section, paired, other).astype(jnp.float32)
    from_previous = jnp.where(even_section, other, paired).astype(jnp.float32)
    pinned = jnp.pad(initial[:, None], ((0, 0), (halo, 0), (0, 0)))
    pinned = jnp.stack([pinned, jnp.zeros_like(pinned)])
    from_previous = jnp.where(is_first, pinned, from_previous)
    extra = from_previous[0, :, 0]
    goal = jnp.concatenate([goal, from_next[0, :, :halo], from_previous[0, :, 1:]], 1)
    inverse = jnp.concatenate([inverse, from_next[1, :, :halo], from_previous[1, :, 1:]], 1)

    def stencil(padded):
        centre = padded[1:-1]
        grid = centre.reshape(-1, GY, GZ)
        total = padded[2:] + padded[:-2]
        in_y = jnp.pad(grid, ((0, 0), (1, 1), (0, 0)))
        in_z = jnp.pad(grid, ((0, 0), (0, 0), (1, 1)))
        total += (in_y[:, 2:] + in_y[:, :-2] + in_z[:, :, 2:] + in_z[:, :, :-2]).reshape(centre.shape)
        return (1.0 - 6.0 * diffusion) * centre + diffusion * total

    moved = stencil(initial)
    extra_moved = jnp.broadcast_to(stencil(extra)[:, None], (planes, 8, plane_size))
    first = jnp.where(is_first, -moved, 0.0)
    target = jnp.concatenate(
        [first[:, None], jnp.zeros((planes, rows - 1, plane_size), jnp.float32)], 1
    )
    first_low = first.astype(jnp.bfloat16)
    first_part = jnp.dot(
        jnp.broadcast_to(first_low.reshape(1, -1), (8, planes * plane_size)),
        input_matrix.reshape(planes * plane_size, width),
        preferred_element_type=jnp.float32,
    )
    part = jnp.concatenate(
        [first_part[:1], jnp.zeros((rows - 1, width), jnp.float32)], 0
    ).astype(jnp.bfloat16)
    rims = target.astype(jnp.bfloat16)
    near_rim = jnp.where(even, rims[planes - 2 :], rims[:2])
    far_rim = jnp.where(even, rims[:2], rims[planes - 2 :])

    states = jnp.zeros((planes + 2, rows, plane_size), jnp.float32)
    duals = jnp.zeros((planes, rows, plane_size), jnp.float32)
    boxed = jnp.zeros((rows, width), jnp.float32)
    scaled = jnp.zeros((rows, width), jnp.float32)
    bound = input_bound.reshape(1, width)

    f32 = jnp.float32
    shape = jax.ShapeDtypeStruct
    vector = shape((8, LANES), f32)
    small = shape((rows, width), f32)
    rim_shape = shape((2, rows, plane_size), jnp.bfloat16)
    flops = 4 * rows * width * planes * plane_size
    primals = []
    gaps = []
    turned_matrix = turned(input_matrix)
    near_matrix = turned(near_matrix)
    far_matrix = turned(far_matrix)
    for iteration in range(ITERS):
        parts = [part] + [swapped(part, "state", mask) for mask in range(1, groups)]
        near_in = swapped(near_rim, "state", 1)
        far_in = across_odd(far_rim, "state")
        head = (*parts, boxed, scaled, bound, kkt_inverse)
        body = (turned_matrix, near_matrix, far_matrix, target, near_in, far_in)
        if iteration < ITERS - 1:
            with_extra = iteration == 0
            tail = (states, duals, inverse, goal) + ((extra_moved,) if with_extra else ())
            outs = (
                small,
                small,
                shape(states.shape, f32),
                shape(duals.shape, f32),
                shape(target.shape, f32),
                shape((rows, width), jnp.bfloat16),
                rim_shape,
                rim_shape,
                vector,
                shape((8, width), f32),
            )
            boxed, scaled, states, duals, target, part, near_rim, far_rim, primal, gap = call(
                functools.partial(step_kernel, groups, own, halo, penalty, with_extra),
                flags,
                (*head, input_matrix, *body, *tail),
                outs,
                [
                    pltpu.VMEM((planes + 4, rows, plane_size), f32),
                    pltpu.VMEM((planes, rows, plane_size), jnp.bfloat16),
                ],
                flops,
            )
        else:
            defect_shape = (planes + 4, rows, plane_size)
            boxed, gap, defect, edge = call(
                functools.partial(last_inputs_kernel, groups, own, penalty),
                flags,
                head + body,
                (
                    small,
                    shape((8, width), f32),
                    shape(defect_shape, f32),
                    shape((planes + 4, 8, plane_size), f32),
                ),
                (),
                flops // 2,
            )
            edge = edge[:, 0]
            following = jnp.where(
                even_section, swapped(edge, "section", 1), across_odd(edge, "section")
            )
            following = jnp.where(is_last, 0.0, following)
            following = jnp.broadcast_to(following[:, None], (planes + 4, 8, plane_size))
            own_shape = shape((planes, own, plane_size), f32)
            states, duals, primal = call(
                functools.partial(last_states_kernel, own),
                None,
                (defect, following, states, duals, inverse, goal),
                (own_shape, own_shape, vector),
                (),
                1_000_000,
            )
        primals.append(primal)
        gaps.append(gap)

    primal_square = jnp.sum(jnp.stack(primals), (1, 2))
    gap_square = jnp.sum(jnp.stack(gaps), (1, 2)) / groups
    totals = jnp.stack([primal_square, gap_square], 1)
    totals = jnp.pad(totals.reshape(1, -1), ((0, 7), (0, LANES - 2 * ITERS)))
    totals = all_sum(all_sum(totals, "state"), "section")
    totals = totals[0, : 2 * ITERS].reshape(ITERS, 2)
    total_sections = own * sections
    counts = jnp.array([total_sections * GX * GY * GZ, total_sections * width], f32)
    record = jnp.sqrt(totals / counts + epsilon)
    return (
        states.transpose(1, 0, 2),
        boxed[:own],
        duals.transpose(1, 0, 2),
        record,
    )


def solution(mesh):
    return jax.shard_map(
        local,
        mesh=mesh,
        in_specs=(
            P("state", None),
            P("section", "state", None),
            P("section", "state", None),
            P("state", None, None),
            P(),
            P(),
        ),
        out_specs=(
            P("section", "state", None),
            P("section", None),
            P("section", "state", None),
            P(),
        ),
        check_vma=False,
    )
```

```python
import functools

import jax
import jax.numpy as jnp
from jax import lax
from jax.experimental import pallas as pl
from jax.experimental.pallas import tpu as pltpu
from jax.sharding import PartitionSpec as P

GX = 32
GY = 32
GZ = 32
ITERS = 10
LANES = 128

diffusion = 0.15
epsilon = 1e-06

VMEM_LIMIT = 14 * 1024 * 1024


def xor_pairs(count, mask):
    return [(i, i ^ mask) for i in range(count)]


def odd_masks(count):
    return sorted({i ^ (i + 1) for i in range(1, count - 1, 2)})


def swapped(value, axis, mask):
    return lax.ppermute(value, axis, xor_pairs(lax.axis_size(axis), mask))


def across_odd(values, axis):
    count = lax.axis_size(axis)
    masks = odd_masks(count)
    if len(masks) == 1:
        return swapped(values, axis, masks[0])
    seat = lax.axis_index(axis)
    result = jnp.zeros_like(values)
    for mask in masks:
        got = swapped(values, axis, mask)
        lower = seat ^ mask
        near = (seat % 2 == 1) & (lower == seat + 1) | (seat % 2 == 0) & (lower + 1 == seat)
        result = jnp.where(near, got, result)
    return result


def bulk_across_odd(value, axis):
    count = lax.axis_size(axis)
    pairs = []
    for i in range(1, count - 1, 2):
        pairs += [(i, i + 1), (i + 1, i)]
    if not pairs:
        return jnp.zeros_like(value)
    return lax.ppermute(value, axis, pairs)


def lane_masks(rows):
    lane = lax.broadcasted_iota(jnp.int32, (rows, LANES), 1)
    return lane < GZ, lane >= LANES - GZ, lane % GZ == 0, lane % GZ == GZ - 1


def stencil_columns(read, columns, masks):
    first_y, last_y, first_z, last_z = masks
    centre = read(0, 0)
    above = 0.0
    up = pltpu.roll(centre, GZ, 1)
    down = pltpu.roll(centre, LANES - GZ, 1)
    for j in range(columns):
        if j < columns - 1:
            centre_next = read(0, j + 1)
            up_next = pltpu.roll(centre_next, GZ, 1)
            down_next = pltpu.roll(centre_next, LANES - GZ, 1)
            below = down_next
        else:
            below = 0.0
        total = jnp.where(first_y, above, up) + jnp.where(last_y, below, down)
        total += jnp.where(first_z, 0.0, pltpu.roll(centre, 1, 1))
        total += jnp.where(last_z, 0.0, pltpu.roll(centre, LANES - 1, 1))
        total += read(-1, j) + read(1, j)
        yield j, centre, (1.0 - 6.0 * diffusion) * centre + diffusion * total
        if j < columns - 1:
            above, centre, up, down = up, centre_next, up_next, down_next


def column(j):
    return slice(j * LANES, (j + 1) * LANES)


def inputs_step(parts, boxed_ref, scaled_ref, bound_ref, kkt_high, kkt_low, penalty, own):
    sums = [p[...].astype(jnp.float32) for p in parts]
    while len(sums) > 1:
        sums = [sums[i] + sums[i + 1] for i in range(0, len(sums), 2)]
    boxed = boxed_ref[...]
    scaled = scaled_ref[...]
    rhs = sums[0] + penalty * (boxed - scaled)
    rhs_high = rhs.astype(jnp.bfloat16)
    rhs_low = (rhs - rhs_high.astype(jnp.float32)).astype(jnp.bfloat16)
    both = jnp.concatenate([rhs_high, rhs_low])
    product = jnp.dot(both, kkt_high[...], preferred_element_type=jnp.float32)
    inputs = product[: rhs.shape[0]] + product[rhs.shape[0] :]
    inputs += jnp.dot(rhs_high, kkt_low[...], preferred_element_type=jnp.float32)
    bound = bound_ref[...]
    boxed_new = jnp.clip(inputs + scaled, -bound, bound)
    gap = inputs - boxed_new
    square = gap * gap
    total = square[0:8]
    for i in range(8, own, 8):
        total = total + square[i : i + 8]
    return inputs, boxed_new, scaled + gap, total


def drive(inputs_low, block):
    return jnp.dot(inputs_low, block, preferred_element_type=jnp.float32)


def rim_defects(flags, inputs_low, near_ref, far_ref, planes, near_rim, far_rim, defect_ref):
    even = flags[0]
    keep = flags[1].astype(jnp.float32)
    near_base = even * (planes + 2)
    far_base = (1 - even) * (planes + 2)
    for i in range(2):
        defect_ref[near_base + i] = near_rim[i].astype(jnp.float32) - drive(inputs_low, near_ref[i])
        defect_ref[far_base + i] = keep * (
            far_rim[i].astype(jnp.float32) - drive(inputs_low, far_ref[i])
        )


def updated_states(q, centre, defect_ref, refs, outs, places, masks, own, keep_duals, total):
    states_ref, duals_ref, inverse_ref, goal_ref = refs
    states_out, duals_out = outs
    state_place, dual_place = places
    columns = states_ref.shape[2] // LANES
    rows = states_ref.shape[1]

    def read(offset, j):
        return defect_ref[centre + offset, :, column(j)]

    for j, defect, spread in stencil_columns(read, columns, masks):
        ahead = pltpu.roll(spread, rows - 1, 0)
        old = states_ref[q, :, column(j)]
        new = goal_ref[q, :, column(j)] + inverse_ref[q, :, column(j)] * (
            (old - defect) + ahead + old
        )
        states_out[state_place, :, column(j)] = new
        if keep_duals:
            dual = (new - old) + defect
            primal = dual - duals_ref[q - 1, :, column(j)]
            duals_out[dual_place, :, column(j)] = dual
            square = primal * primal
            for i in range(0, own, 8):
                total = total + square[i : i + 8]
    return total


def own_kernel(groups, own, penalty, *refs):
    parts, refs = refs[:groups], refs[groups:]
    boxed_ref, scaled_ref, bound_ref, kkt_high, kkt_low, turned_ref, target_ref, *costs = refs[:11]
    boxed_out, scaled_out, gap_out, low_out = refs[11:15]
    states_out, duals_out, edge_out, primal_out, defect_ref = refs[15:]
    planes, rows, plane_size = target_ref.shape
    inputs, boxed_out[...], scaled_out[...], gap_out[...] = inputs_step(
        parts, boxed_ref, scaled_ref, bound_ref, kkt_high, kkt_low, penalty, own
    )
    inputs_low = inputs.astype(jnp.bfloat16)
    low_out[...] = inputs_low
    masks = lane_masks(rows)

    def own_defect(p, carry):
        defect_ref[p] = target_ref[p] - drive(inputs_low, turned_ref[p])
        return carry

    def states_and_defect(q, total):
        total = updated_states(
            q, q - 1, defect_ref, costs, (states_out, duals_out), (q - 2, q - 2), masks, own, True, total
        )
        return own_defect(jnp.minimum(q + 1, planes - 1), total)

    lax.fori_loop(0, 3, own_defect, 0)
    primal_out[...] = lax.fori_loop(
        2, planes, states_and_defect, jnp.zeros((8, LANES), jnp.float32)
    )
    for i in range(2):
        edge_out[i] = defect_ref[i]
        edge_out[2 + i] = defect_ref[planes - 2 + i]


def rims_kernel(own, halo, with_extra, *refs):
    flags, low_ref_in, near_ref, far_ref, near_rim, far_rim, edge_ref, mid_states, mid_duals = refs[:9]
    costs = refs[9:13]
    matrix_ref = refs[13]
    refs = list(refs[14:])
    extra_ref = refs.pop(0) if with_extra else None
    states_out, duals_out, target_out, part_out, near_out, far_out, primal_out = refs[:7]
    defect_ref, low_ref = refs[7:]
    planes, rows, plane_size = target_out.shape
    columns = plane_size // LANES
    masks = lane_masks(rows)
    even = flags[0]
    keep = flags[1].astype(jnp.float32)
    inputs_low = low_ref_in[...]
    near_base = even * 6
    far_base = (1 - even) * 6

    def rim_defect(i, carry):
        defect_ref[near_base + i] = near_rim[i].astype(jnp.float32) - drive(inputs_low, near_ref[i])
        defect_ref[far_base + i] = keep * (
            far_rim[i].astype(jnp.float32) - drive(inputs_low, far_ref[i])
        )
        defect_ref[2 + i] = edge_ref[i]
        defect_ref[4 + i] = edge_ref[2 + i]
        return carry

    def carried(i, carry):
        states_out[i + 2] = mid_states[i]
        duals_out[i + 1] = mid_duals[i]
        return carry

    def edge_states(side, total):
        outs = (states_out, duals_out)
        outer = side * (planes + 1)
        updated_states(
            outer, 1 + 5 * side, defect_ref, costs, outs, (outer, 0), masks, own, False, total
        )
        inner = 1 + side * (planes - 1)
        return updated_states(
            inner, 2 + 3 * side, defect_ref, costs, outs, (inner, inner - 1), masks, own, True, total
        )

    lax.fori_loop(0, 2, rim_defect, 0)
    lax.fori_loop(0, planes - 2, carried, 0)
    primal_out[...] = lax.fori_loop(0, 2, edge_states, jnp.zeros((8, LANES), jnp.float32))

    row = lax.broadcasted_iota(jnp.int32, (rows, LANES), 0)
    live = (row < own) | (row < own + halo) & (flags[3] == 0) | (row >= own + halo) & (flags[2] == 0)

    def pull(p):
        return jnp.dot(
            low_ref[p], matrix_ref[jnp.maximum(p - 1, 0)], preferred_element_type=jnp.float32
        )

    def pull_and_target(p, part):
        part = part + pull(p)

        def read(offset, j):
            block = states_out[p + 1 + offset, :, column(j)]
            if with_extra:
                before = extra_ref[p + 1 + offset, 0:1, column(j)]
                block = jnp.where(row == own + halo, before, pltpu.roll(block, 1, 0))
            return block

        for j, _, spread in stencil_columns(read, columns, masks):
            moved = spread if with_extra else pltpu.roll(spread, 1, 0)
            new = (states_out[p + 1, :, column(j)] - moved) + duals_out[p, :, column(j)]
            new = jnp.where(live, new, 0.0)
            target_out[p, :, column(j)] = new
            low_ref[p + 1, :, column(j)] = new.astype(jnp.bfloat16)
        return part

    width = matrix_ref.shape[2]
    low_ref[0] = jnp.zeros((rows, plane_size), jnp.bfloat16)
    part = lax.fori_loop(0, planes, pull_and_target, jnp.zeros((rows, width), jnp.float32))
    part_out[...] = (part + pull(planes)).astype(jnp.bfloat16)
    near_base = 1 + even * (planes - 2)
    far_base = 1 + (1 - even) * (planes - 2)
    for i in range(2):
        near_out[i] = low_ref[near_base + i]
        far_out[i] = low_ref[far_base + i]


def first_kernel(flags, initial_ref, matrix_ref, target_out, part_out, near_out, far_out, low_ref):
    planes, rows, plane_size = target_out.shape
    columns = plane_size // LANES
    masks = lane_masks(8)
    live = (lax.broadcasted_iota(jnp.int32, (8, LANES), 0) == 0) & (flags[2] == 1)
    rest = jnp.zeros((rows - 8, LANES), jnp.float32)

    def body(p, part):
        def read(offset, j):
            return jnp.broadcast_to(initial_ref[p + 1 + offset, 0:1, column(j)], (8, LANES))

        for j, _, spread in stencil_columns(read, columns, masks):
            new = jnp.concatenate([jnp.where(live, -spread, 0.0), rest])
            target_out[p, :, column(j)] = new
            low_ref[p, :, column(j)] = new.astype(jnp.bfloat16)
        return part + jnp.dot(low_ref[p], matrix_ref[p], preferred_element_type=jnp.float32)

    width = matrix_ref.shape[2]
    part = lax.fori_loop(0, planes, body, jnp.zeros((rows, width), jnp.float32))
    part_out[...] = part.astype(jnp.bfloat16)
    near_base = flags[0] * (planes - 2)
    far_base = (1 - flags[0]) * (planes - 2)
    for i in range(2):
        near_out[i] = low_ref[near_base + i]
        far_out[i] = low_ref[far_base + i]


def turn_kernel(block_ref, out_ref):
    out_ref[0] = block_ref[0].T


def turn_rims_kernel(near_ref, far_ref, near_out, far_out):
    for i in range(near_ref.shape[0]):
        near_out[i] = near_ref[i].T
        far_out[i] = far_ref[i].T


def turned(matrix):
    count, height, width = matrix.shape
    return pl.pallas_call(
        turn_kernel,
        grid=(count,),
        out_shape=jax.ShapeDtypeStruct((count, width, height), matrix.dtype),
        in_specs=[pl.BlockSpec((1, height, width), lambda p: (p, 0, 0))],
        out_specs=pl.BlockSpec((1, width, height), lambda p: (p, 0, 0)),
        compiler_params=pltpu.CompilerParams(vmem_limit_bytes=VMEM_LIMIT),
        cost_estimate=pl.CostEstimate(
            flops=50 * count * height * width, bytes_accessed=4 * count * height * width, transcendentals=0
        ),
    )(matrix)


def last_inputs_kernel(groups, own, penalty, *refs):
    refs = list(refs)
    flags = refs.pop(0)
    parts = [refs.pop(0) for _ in range(groups)]
    boxed_ref, scaled_ref, bound_ref, kkt_high, kkt_low = [refs.pop(0) for _ in range(5)]
    turned_ref, near_ref, far_ref = [refs.pop(0) for _ in range(3)]
    target_ref, near_rim, far_rim = [refs.pop(0) for _ in range(3)]
    boxed_out, gap_out, defect_out, first_out = refs
    inputs, boxed_new, _, gap_total = inputs_step(
        parts, boxed_ref, scaled_ref, bound_ref, kkt_high, kkt_low, penalty, own
    )
    boxed_out[...] = boxed_new
    gap_out[...] = gap_total
    inputs_low = inputs.astype(jnp.bfloat16)
    planes = target_ref.shape[0]
    rim_defects(flags, inputs_low, near_ref, far_ref, planes, near_rim, far_rim, defect_out)

    def own_defect(p, _):
        defect_out[p + 2] = target_ref[p] - drive(inputs_low, turned_ref[p])
        return 0

    lax.fori_loop(0, planes, own_defect, 0)
    first_out[...] = defect_out[:, 0:8, :]


def last_states_kernel(
    own, defect_ref, following_ref, states_ref, duals_ref, inverse_ref, goal_ref, *outs
):
    states_out, duals_out, primal_out = outs
    planes = states_out.shape[0]
    columns = states_out.shape[2] // LANES
    masks = lane_masks(own)
    last = lax.broadcasted_iota(jnp.int32, (own, LANES), 0) == own - 1

    def body(p, total):
        def read(offset, j):
            own_rows = defect_ref[p + 2 + offset, 0:own, column(j)]
            after = following_ref[p + 2 + offset, 0:1, column(j)]
            return jnp.where(last, after, pltpu.roll(own_rows, own - 1, 0))

        for j, _, spread in stencil_columns(read, columns, masks):
            defect = defect_ref[p + 2, 0:own, column(j)]
            old = states_ref[p + 1, 0:own, column(j)]
            new = goal_ref[p + 1, 0:own, column(j)] + inverse_ref[p + 1, 0:own, column(j)] * (
                (old - defect) + spread + old
            )
            dual = (new - old) + defect
            primal = dual - duals_ref[p, 0:own, column(j)]
            states_out[p, :, column(j)] = new
            duals_out[p, :, column(j)] = dual
            square = primal * primal
            for i in range(0, own, 8):
                total = total + square[i : i + 8]
        return total

    primal_out[...] = lax.fori_loop(0, planes, body, jnp.zeros((8, LANES), jnp.float32))


def in_vmem(count):
    return [pl.BlockSpec(memory_space=pltpu.VMEM)] * count


def call(kernel, flags, operands, outs, scratch=(), flops=0):
    specs = in_vmem(len(operands))
    if flags is not None:
        specs = [pl.BlockSpec(memory_space=pltpu.SMEM)] + specs
        operands = (flags, *operands)
    return pl.pallas_call(
        kernel,
        out_shape=outs,
        in_specs=specs,
        out_specs=tuple(in_vmem(len(outs))),
        scratch_shapes=list(scratch),
        compiler_params=pltpu.CompilerParams(vmem_limit_bytes=VMEM_LIMIT),
        cost_estimate=pl.CostEstimate(flops=flops, bytes_accessed=30_000_000, transcendentals=0),
    )(*operands)


def all_sum(value, axis):
    mask = 1
    while mask < lax.axis_size(axis):
        value = value + swapped(value, axis, mask)
        mask *= 2
    return value


def local(initial_state, state_ref, state_weight, input_matrix, kkt_inverse, input_bound):
    own, planes, plane_size = state_ref.shape
    width = input_matrix.shape[2]
    halo = ITERS - 2
    rows = own + 2 * halo
    assert own > halo and own % 8 == 0 and halo % 8 == 0 and plane_size == GY * GZ
    penalty = float(GX * GY * GZ) / width
    groups = lax.axis_size("state")
    sections = lax.axis_size("section")
    seat = lax.axis_index("state")
    section = lax.axis_index("section")
    even = seat % 2 == 0
    even_section = section % 2 == 0
    is_first = section == 0
    is_last = section == sections - 1
    far_lives = jnp.logical_not((seat == 0) | (seat == groups - 1) & (groups % 2 == 0))
    flags = jnp.stack(
        [even.astype(jnp.int32), far_lives.astype(jnp.int32), is_first.astype(jnp.int32), is_last.astype(jnp.int32)]
    )

    def costs(weight, goal):
        inverse = 1.0 / (weight + 2.0)
        return weight * goal * inverse, inverse

    def rim_costs(plane):
        return jnp.concatenate(
            [*costs(state_weight[:, plane], state_ref[:, plane]), initial_state[plane : plane + 1]]
        )

    above = rim_costs(planes - 1)
    below = rim_costs(0)
    near_plane = jnp.where(even, above, below).astype(jnp.bfloat16)
    far_plane = jnp.where(even, below, above).astype(jnp.bfloat16)
    base = jnp.where(even, planes - 2, 0)
    near_plane, far_plane, base, state_weight, state_ref = lax.optimization_barrier(
        (near_plane, far_plane, base, state_weight, state_ref)
    )
    near_plane = swapped(near_plane, "state", 1)
    far_plane = across_odd(far_plane, "state")

    far_matrix = lax.dynamic_slice_in_dim(input_matrix, planes - 2 - base, 2)
    far_matrix, base = lax.optimization_barrier((far_matrix, base))
    far_matrix = bulk_across_odd(far_matrix, "state")
    near_matrix = swapped(lax.dynamic_slice_in_dim(input_matrix, base, 2), "state", 1)

    near_plane = near_plane.astype(jnp.float32)
    far_plane = jnp.where(far_lives, far_plane.astype(jnp.float32), 0.0)
    low_plane = jnp.where(even, far_plane, near_plane)
    high_plane = jnp.where(even, near_plane, far_plane)

    def with_rims(low, block, high):
        return jnp.concatenate([low[None], block, high[None]])

    goal, inverse = costs(state_weight, state_ref)
    goal = with_rims(low_plane[:own], goal.transpose(1, 0, 2), high_plane[:own])
    inverse = with_rims(
        low_plane[own : 2 * own], inverse.transpose(1, 0, 2), high_plane[own : 2 * own]
    )
    initial = with_rims(low_plane[2 * own], initial_state, high_plane[2 * own])

    def message(first, stop):
        return jnp.stack([goal[:, first:stop], inverse[:, first:stop]]).astype(jnp.bfloat16)

    to_next = message(own - halo - 1, own)
    to_previous = message(0, halo + 1)
    paired = swapped(jnp.where(even_section, to_next, to_previous), "section", 1)
    other = bulk_across_odd(jnp.where(even_section, to_previous, to_next), "section")
    from_next = jnp.where(even_section, paired, other).astype(jnp.float32)
    from_previous = jnp.where(even_section, other, paired).astype(jnp.float32)
    pinned = jnp.pad(initial[:, None], ((0, 0), (halo, 0), (0, 0)))
    pinned = jnp.stack([pinned, jnp.zeros_like(pinned)])
    from_previous = jnp.where(is_first, pinned, from_previous)
    extra = from_previous[0, :, 0]
    goal = jnp.concatenate([goal, from_next[0, :, :halo], from_previous[0, :, 1:]], 1)
    inverse = jnp.concatenate([inverse, from_next[1, :, :halo], from_previous[1, :, 1:]], 1)

    states = jnp.zeros((planes + 2, rows, plane_size), jnp.float32)
    duals = jnp.zeros((planes, rows, plane_size), jnp.float32)
    boxed = jnp.zeros((rows, width), jnp.float32)
    scaled = jnp.zeros((rows, width), jnp.float32)
    bound = input_bound.reshape(1, width)

    f32 = jnp.float32
    shape = jax.ShapeDtypeStruct
    vector = shape((8, LANES), f32)
    small = shape((rows, width), f32)
    rim_shape = shape((2, rows, plane_size), jnp.bfloat16)
    flops = 4 * rows * width * planes * plane_size
    primals = []
    gaps = []
    turned_matrix = turned(input_matrix)
    turned_rim = shape((2, width, plane_size), input_matrix.dtype)
    near_matrix, far_matrix = call(
        turn_rims_kernel, None, (near_matrix, far_matrix), (turned_rim, turned_rim), (), flops // 8
    )
    kkt_high = lax.reduce_precision(kkt_inverse, 8, 7)
    kkt_low = (kkt_inverse - kkt_high).astype(jnp.bfloat16)
    kkt_high = kkt_high.astype(jnp.bfloat16)
    target_shape = shape((planes, rows, plane_size), f32)
    low_shape = pltpu.VMEM((planes, rows, plane_size), jnp.bfloat16)
    part_shape = shape((rows, width), jnp.bfloat16)
    target, part, near_rim, far_rim = call(
        first_kernel,
        flags,
        (initial[:, None], input_matrix),
        (target_shape, part_shape, rim_shape, rim_shape),
        [low_shape],
        flops // 2,
    )
    for iteration in range(ITERS):
        parts = [part] + [swapped(part, "state", mask) for mask in range(1, groups)]
        near_in = swapped(near_rim, "state", 1)
        far_in = across_odd(far_rim, "state")
        head = (*parts, boxed, scaled, bound, kkt_high, kkt_low, turned_matrix)
        if iteration < ITERS - 1:
            with_extra = iteration == 0
            boxed, scaled, gap, inputs_low, mid_states, mid_duals, edge, primal = call(
                functools.partial(own_kernel, groups, own, penalty),
                None,
                (*head, target, states, duals, inverse, goal),
                (
                    small,
                    small,
                    shape((8, width), f32),
                    part_shape,
                    shape((planes - 2, rows, plane_size), f32),
                    shape((planes - 2, rows, plane_size), f32),
                    shape((4, rows, plane_size), f32),
                    vector,
                ),
                [pltpu.VMEM(target_shape.shape, f32)],
                flops // 2,
            )
            states, duals, target, part, near_rim, far_rim, primal_edge = call(
                functools.partial(rims_kernel, own, halo, with_extra),
                flags,
                (
                    inputs_low,
                    near_matrix,
                    far_matrix,
                    near_in,
                    far_in,
                    edge,
                    mid_states,
                    mid_duals,
                    states,
                    duals,
                    inverse,
                    goal,
                    input_matrix,
                )
                + ((extra[:, None],) if with_extra else ()),
                (
                    shape(states.shape, f32),
                    shape(duals.shape, f32),
                    target_shape,
                    part_shape,
                    rim_shape,
                    rim_shape,
                    vector,
                ),
                [
                    pltpu.VMEM((8, rows, plane_size), f32),
                    pltpu.VMEM((planes + 1, rows, plane_size), jnp.bfloat16),
                ],
                flops // 2,
            )
            primals.append(primal_edge)
        else:
            defect_shape = (planes + 4, rows, plane_size)
            boxed, gap, defect, edge = call(
                functools.partial(last_inputs_kernel, groups, own, penalty),
                flags,
                (*head, near_matrix, far_matrix, target, near_in, far_in),
                (
                    small,
                    shape((8, width), f32),
                    shape(defect_shape, f32),
                    shape((planes + 4, 8, plane_size), f32),
                ),
                (),
                flops // 2,
            )
            edge = edge[:, 0]
            following = jnp.where(
                even_section, swapped(edge, "section", 1), across_odd(edge, "section")
            )
            following = jnp.where(is_last, 0.0, following)
            following = jnp.broadcast_to(following[:, None], (planes + 4, 8, plane_size))
            own_shape = shape((planes, own, plane_size), f32)
            states, duals, primal = call(
                functools.partial(last_states_kernel, own),
                None,
                (defect, following, states, duals, inverse, goal),
                (own_shape, own_shape, vector),
                (),
                1_000_000,
            )
        primals.append(primal)
        gaps.append(gap)

    primals = [sum(primals[i : i + 2]) for i in range(0, len(primals), 2)]
    primal_square = jnp.sum(jnp.stack(primals), (1, 2))
    gap_square = jnp.sum(jnp.stack(gaps), (1, 2)) / groups
    totals = jnp.stack([primal_square, gap_square], 1)
    totals = jnp.pad(totals.reshape(1, -1), ((0, 7), (0, LANES - 2 * ITERS)))
    totals = all_sum(all_sum(totals, "state"), "section")
    totals = totals[0, : 2 * ITERS].reshape(ITERS, 2)
    total_sections = own * sections
    counts = jnp.array([total_sections * GX * GY * GZ, total_sections * width], f32)
    record = jnp.sqrt(totals / counts + epsilon)
    return (
        states.transpose(1, 0, 2),
        boxed[:own],
        duals.transpose(1, 0, 2),
        record,
    )


def solution(mesh):
    return jax.shard_map(
        local,
        mesh=mesh,
        in_specs=(
            P("state", None),
            P("section", "state", None),
            P("section", "state", None),
            P("state", None, None),
            P(),
            P(),
        ),
        out_specs=(
            P("section", "state", None),
            P("section", None),
            P("section", "state", None),
            P(),
        ),
        check_vma=False,
    )
```
